32 devices in a mesh: dp: 2 (over x), sp: 4 (over z), tp: 4 (over y, core).
Axes of the slice: x: 2, y: 2, z: 4, core: 2. Of those that a mesh axis runs over, the one named last changes fastest.
Arguments:
- x: bfloat16 [8192, 4096], P(('dp', 'sp', 'tp')), parts along dimension 0
- segment_ids: int32 [8192], P(('dp', 'sp', 'tp')), parts along dimension 0
- positions: int32 [8192], P(('dp', 'sp', 'tp')), parts along dimension 0
- g_attn: bfloat16 [2, 4096], replicated
- w_q: bfloat16 [2, 4096, 32, 128], P(None, None, 'tp')
- w_k: bfloat16 [2, 4096, 8, 128], replicated
- w_v: bfloat16 [2, 4096, 8, 128], replicated
- w_o: bfloat16 [2, 32, 128, 4096], P(None, 'tp')
- g_mlp: bfloat16 [2, 4096], replicated
- w_gate: bfloat16 [2, 4096, 14336], P(None, None, 'tp')
- w_up: bfloat16 [2, 4096, 14336], P(None, None, 'tp')
- w_down: bfloat16 [2, 14336, 4096], P(None, 'tp')
Outputs:
- output: bfloat16 [8192, 4096], P(('dp', 'sp', 'tp')), parts along dimension 0
There are 2 independent parts. The reference program is written for one: setup_inputs(seed, part) draws one part's arguments, and reference() takes and returns one part's arrays. A program takes and returns all parts, laid end to end along the dimension named above; an argument that names none is the same for every part.
All inputs are finite; a program needn't handle non-finite values.
Results may differ from the reference program's by a relative error of at most 0.0180036.
Values are sent between devices in bfloat16 or wider.
A program may use at most 1 GiB of HBM per device.

```python
import jax
import jax.numpy as jnp
from jax import lax

D = 4096
HEADS = 32
KV_HEADS = 8
HEAD = 128
FF = 14336
LAYERS = 2
TOKENS = 4096
WINDOW = 1024
ROPE_BASE = 10000
EPS = 1e-6
REF_ROWS = max(1024 // HEADS, 8)
GROUP = HEADS // KV_HEADS


def draw_layout(layout_key):
    k_first, k_second, k_step, k_offset = jax.random.split(layout_key, 4)
    first_cut = jax.random.randint(k_first, (), TOKENS // 2, 3 * TOKENS // 4)
    second_cut = jax.random.randint(k_second, (), first_cut + TOKENS // 16, TOKENS - TOKENS // 16 + 1)
    tok_index = jnp.arange(TOKENS)
    segment_ids = (tok_index >= first_cut).astype(jnp.int32) + (tok_index >= second_cut).astype(jnp.int32)
    step_sizes = jax.random.randint(k_step, (TOKENS,), 1, 8)
    before = jnp.cumsum(step_sizes) - step_sizes
    seg_starts = before[jnp.stack([jnp.zeros((), first_cut.dtype), first_cut, second_cut])]
    seg_offsets = jax.random.randint(k_offset, (3,), 0, 512)
    positions = before - seg_starts[segment_ids] + seg_offsets[segment_ids]
    return segment_ids, positions.astype(jnp.int32)


def draw_stack(stack_key, shape, scale):
    layer_keys = jax.random.split(stack_key, LAYERS)
    return lax.map(lambda one_key: (jax.random.normal(one_key, shape, jnp.float32) * scale).astype(jnp.bfloat16), layer_keys)


def setup_inputs(seed: int = 0, part: int = 0) -> dict:
    root_key = jax.random.key(seed)
    part_key = jax.random.fold_in(root_key, part)
    k_layout, k_noise, k_walk = jax.random.split(part_key, 3)
    segment_ids, positions = draw_layout(k_layout)
    noise = jax.random.normal(k_noise, (TOKENS, D), jnp.float32)
    walk = jnp.cumsum(jax.random.normal(k_walk, (TOKENS, D), jnp.float32), axis=0) * (1.5 / TOKENS ** 0.5)
    x = (0.6 * noise + walk).astype(jnp.bfloat16)
    w_keys = jax.random.split(jax.random.key(seed + 1), 8)
    gains = 1.0 + 0.5 * jax.random.normal(w_keys[0], (2, LAYERS, D), jnp.float32)
    return {
        "x": x,
        "segment_ids": segment_ids,
        "positions": positions,
        "g_attn": gains[0].astype(jnp.bfloat16),
        "w_q": draw_stack(w_keys[1], (D, HEADS, HEAD), D ** -0.5),
        "w_k": draw_stack(w_keys[2], (D, KV_HEADS, HEAD), D ** -0.5),
        "w_v": draw_stack(w_keys[3], (D, KV_HEADS, HEAD), D ** -0.5),
        "w_o": draw_stack(w_keys[4], (HEADS, HEAD, D), (HEADS * HEAD) ** -0.5),
        "g_mlp": gains[1].astype(jnp.bfloat16),
        "w_gate": draw_stack(w_keys[5], (D, FF), D ** -0.5),
        "w_up": draw_stack(w_keys[6], (D, FF), D ** -0.5),
        "w_down": draw_stack(w_keys[7], (FF, D), FF ** -0.5),
    }


def rms_norm(x, gain):
    x_wide = x.astype(jnp.float32)
    inv_rms = lax.rsqrt(jnp.mean(x_wide * x_wide, axis=-1, keepdims=True) + EPS)
    return (x_wide * inv_rms * gain.astype(jnp.float32)).astype(jnp.bfloat16)


def rope(t, cos_tab, sin_tab):
    half_width = HEAD // 2
    t_wide = t.astype(jnp.float32)
    lower_half = t_wide[..., :half_width]
    upper_half = t_wide[..., half_width:]
    return jnp.concatenate([lower_half * cos_tab - upper_half * sin_tab, upper_half * cos_tab + lower_half * sin_tab], axis=-1).astype(jnp.bfloat16)


def attention(q, k, v, segment_ids, windowed):
    block_rows = REF_ROWS
    key_span = min(block_rows + WINDOW, TOKENS) if windowed else TOKENS
    blocks = TOKENS // block_rows
    q_blocks = q.reshape(blocks, block_rows, KV_HEADS, GROUP, HEAD)

    def one_block(block_args):
        q_blk, block_idx = block_args
        q_start = block_idx * block_rows
        k_start = jnp.clip(q_start + block_rows - key_span, 0, TOKENS - key_span)
        k_blk = lax.dynamic_slice_in_dim(k, k_start, key_span, 0)
        v_blk = lax.dynamic_slice_in_dim(v, k_start, key_span, 0)
        seg_q = lax.dynamic_slice_in_dim(segment_ids, q_start, block_rows, 0)
        seg_k = lax.dynamic_slice_in_dim(segment_ids, k_start, key_span, 0)
        q_pos = q_start + jnp.arange(block_rows)
        k_pos = k_start + jnp.arange(key_span)
        allowed = (k_pos[None, :] <= q_pos[:, None]) & (seg_k[None, :] == seg_q[:, None])
        if windowed:
            allowed = allowed & (q_pos[:, None] - k_pos[None, :] < WINDOW)
        scores = jnp.einsum("qgrd,kgd->qgrk", q_blk.astype(jnp.float32), k_blk.astype(jnp.float32)) * HEAD ** -0.5
        scores = jnp.where(allowed[:, None, None, :], scores, -1e30)
        attn_probs = jax.nn.softmax(scores, axis=-1).astype(jnp.bfloat16).astype(jnp.float32)
        mixed = jnp.einsum("qgrk,kgd->qgrd", attn_probs, v_blk.astype(jnp.float32))
        return mixed.astype(jnp.bfloat16)

    out_blocks = lax.map(one_block, (q_blocks, jnp.arange(blocks)))
    return out_blocks.reshape(TOKENS, HEADS * HEAD)


def decoder_layer(x, params, cos_tab, sin_tab, segment_ids, windowed):
    g_attn, w_q, w_k, w_v, w_o, g_mlp, w_gate, w_up, w_down = params
    normed = rms_norm(x, g_attn)
    q = jnp.dot(normed, w_q.reshape(D, HEADS * HEAD), preferred_element_type=jnp.float32).astype(jnp.bfloat16)
    k = jnp.dot(normed, w_k.reshape(D, KV_HEADS * HEAD), preferred_element_type=jnp.float32).astype(jnp.bfloat16)
    v = jnp.dot(normed, w_v.reshape(D, KV_HEADS * HEAD), preferred_element_type=jnp.float32).astype(jnp.bfloat16)
    q = rope(q.reshape(TOKENS, HEADS, HEAD), cos_tab, sin_tab).reshape(TOKENS, KV_HEADS, GROUP, HEAD)
    k = rope(k.reshape(TOKENS, KV_HEADS, HEAD), cos_tab, sin_tab)
    v = v.reshape(TOKENS, KV_HEADS, HEAD)
    mixed = attention(q, k, v, segment_ids, windowed)
    attn_out = jnp.dot(mixed, w_o.reshape(HEADS * HEAD, D), preferred_element_type=jnp.float32).astype(jnp.bfloat16)
    hidden = (x.astype(jnp.float32) + attn_out.astype(jnp.float32)).astype(jnp.bfloat16)
    normed = rms_norm(hidden, g_mlp)
    gate_proj = jnp.dot(normed, w_gate, preferred_element_type=jnp.float32)
    up_proj = jnp.dot(normed, w_up, preferred_element_type=jnp.float32)
    activation = (jax.nn.silu(gate_proj) * up_proj).astype(jnp.bfloat16)
    mlp_out = jnp.dot(activation, w_down, preferred_element_type=jnp.float32).astype(jnp.bfloat16)
    return (hidden.astype(jnp.float32) + mlp_out.astype(jnp.float32)).astype(jnp.bfloat16)


def reference(x, segment_ids, positions, g_attn, w_q, w_k, w_v, w_o, g_mlp, w_gate, w_up, w_down):
    inv_freq = ROPE_BASE ** (-jnp.arange(HEAD // 2, dtype=jnp.float32) / (HEAD // 2))
    angles = positions.astype(jnp.float32)[:, None] * inv_freq[None, :]
    cos_tab = jnp.cos(angles)[:, None, :]
    sin_tab = jnp.sin(angles)[:, None, :]
    stacked = tuple(w.reshape((LAYERS // 2, 2) + w.shape[1:]) for w in (g_attn, w_q, w_k, w_v, w_o, g_mlp, w_gate, w_up, w_down))

    def pair_step(residual, layer_pair):
        residual = decoder_layer(residual, tuple(w[0] for w in layer_pair), cos_tab, sin_tab, segment_ids, True)
        residual = decoder_layer(residual, tuple(w[1] for w in layer_pair), cos_tab, sin_tab, segment_ids, False)
        return residual, None

    final_x, unused_ys = lax.scan(pair_step, x, stacked)
    return final_x
```

```python
import functools

import jax
import jax.numpy as jnp
from jax import lax
from jax.experimental import pallas as pl
from jax.experimental.pallas import tpu as pltpu
from jax.sharding import PartitionSpec as P


EPS = 1e-6
ROPE_BASE = 10000.0
WINDOW = 1024
HEAD = 128
CHUNKS = 2
VMEM = 40 << 20
NEG = -1e30
LOG2E = 1.4426950408889634


def add_round(a, b):
    return (a.astype(jnp.float32) + b.astype(jnp.float32)).astype(jnp.bfloat16)


def relayout_kernel(sc_ref, wq_ref, wk_ref, wv_ref, q_ref, kv_ref, tmp_ref):
    q_ref[...] = pltpu.einshape("khd->k(hd)", wq_ref[0])
    width = kv_ref.shape[1] // 2
    start = pl.multiple_of(sc_ref[0] * width, width)
    for i, w in enumerate((wk_ref, wv_ref)):
        tmp_ref[i] = pltpu.einshape("khd->k(hd)", w[0])
        part = tmp_ref[i, :, pl.ds(start, width)]
        for h in range(width // HEAD):
            at = (2 * h + i) * HEAD
            kv_ref[:, at:at + HEAD] = part[:, h * HEAD:(h + 1) * HEAD]


def relayout(w_q, w_k, w_v, which, layer, kv_loc):
    _, k, heads, _ = w_q.shape
    kv_heads = w_k.shape[2]
    bk = 256
    return pl.pallas_call(
        relayout_kernel,
        grid_spec=pltpu.PrefetchScalarGridSpec(
            num_scalar_prefetch=1,
            grid=(k // bk,),
            in_specs=[pl.BlockSpec((1, bk, heads, HEAD), lambda i, s: (layer, i, 0, 0))]
            + [pl.BlockSpec((1, bk, kv_heads, HEAD), lambda i, s: (layer, i, 0, 0))] * 2,
            out_specs=[pl.BlockSpec((bk, heads * HEAD), lambda i, s: (i, 0)), pl.BlockSpec((bk, 2 * kv_loc * HEAD), lambda i, s: (i, 0))],
            scratch_shapes=[pltpu.VMEM((2, bk, kv_heads * HEAD), jnp.bfloat16)],
        ),
        out_shape=[jax.ShapeDtypeStruct((k, heads * HEAD), jnp.bfloat16), jax.ShapeDtypeStruct((k, 2 * kv_loc * HEAD), jnp.bfloat16)],
        cost_estimate=pl.CostEstimate(flops=10 ** 10, bytes_accessed=8 * k * heads * HEAD, transcendentals=0),
        compiler_params=pltpu.CompilerParams(vmem_limit_bytes=VMEM),
        name="relayout",
    )(which, w_q, w_k, w_v)


def norm_kernel(x_ref, s_ref, r_ref, g_ref, h_ref, n_ref):
    total = (s_ref[...].astype(jnp.float32) + r_ref[...].astype(jnp.float32)).astype(jnp.bfloat16)
    h = (x_ref[...].astype(jnp.float32) + total.astype(jnp.float32)).astype(jnp.bfloat16)
    h_ref[...] = h
    wide = h.astype(jnp.float32)
    inv_rms = lax.rsqrt(jnp.mean(wide * wide, axis=-1, keepdims=True) + EPS)
    n_ref[...] = (wide * inv_rms * g_ref[...]).astype(jnp.bfloat16)


def residual_norm(x, s, r, gain):
    rows, n = x.shape
    part = rows // 2
    here = pl.BlockSpec((part, n), lambda i: (i, 0))
    return pl.pallas_call(
        norm_kernel,
        grid=(2,),
        in_specs=[here, here, pl.BlockSpec((part, n), lambda i: (1 - i, 0)), pl.BlockSpec((1, n), lambda i: (0, 0))],
        out_specs=[here, here],
        out_shape=[jax.ShapeDtypeStruct((rows, n), jnp.bfloat16)] * 2,
        cost_estimate=pl.CostEstimate(flops=10 ** 8, bytes_accessed=10 * rows * n, transcendentals=0),
        compiler_params=pltpu.CompilerParams(vmem_limit_bytes=30 << 20),
        name="residual_norm",
    )(x, s, r, gain.astype(jnp.float32)[None])


def rotate(t, cos, sin):
    wide = t.astype(jnp.float32)
    return (wide * cos + pltpu.roll(wide, HEAD // 2, 1) * sin).astype(jnp.bfloat16)


def q_kernel(*refs):
    xs, (w_ref, cos_ref, sin_ref, o_ref) = refs[:2], refs[2:]
    x = jnp.concatenate([r[...] for r in xs], axis=0)
    t = jnp.dot(x, w_ref[...], preferred_element_type=jnp.float32).astype(jnp.bfloat16)
    for h in range(t.shape[1] // HEAD):
        cols = slice(h * HEAD, (h + 1) * HEAD)
        o_ref[:, cols] = rotate(t[:, cols], cos_ref[...], sin_ref[...])


def kv_kernel(*refs):
    xs, (w_ref, cos_ref, sin_ref), os = refs[:2], refs[2:5], refs[5:]
    step = pl.program_id(0)
    x = jnp.concatenate([r[...] for r in xs], axis=0)
    t = jnp.dot(x, w_ref[...], preferred_element_type=jnp.float32).astype(jnp.bfloat16)
    k = rotate(t[:, :HEAD], cos_ref[...], sin_ref[...])
    for h, o in enumerate(os):
        @pl.when(step == h)
        def _():
            o[:, :HEAD] = k
            o[:, HEAD:] = t[:, HEAD:]


def project(kernel, blocks, weight, cos_t, sin_t, outs):
    rows = sum(b.shape[0] for b in blocks)
    k, n = weight.shape
    bn = 2 * HEAD
    if outs == 1:
        out_specs = pl.BlockSpec((rows, bn), lambda j: (0, j))
        out_shape = jax.ShapeDtypeStruct((rows, n), jnp.bfloat16)
    else:
        out_specs = [pl.BlockSpec((rows, bn), lambda j: (0, 0))] * outs
        out_shape = [jax.ShapeDtypeStruct((rows, bn), jnp.bfloat16)] * outs
    return pl.pallas_call(
        kernel,
        grid=(n // bn,),
        in_specs=[pl.BlockSpec(b.shape, lambda j: (0, 0)) for b in blocks]
        + [pl.BlockSpec((k, bn), lambda j: (0, j))]
        + [pl.BlockSpec(cos_t.shape, lambda j: (0, 0))] * 2,
        out_specs=out_specs,
        out_shape=out_shape,
        cost_estimate=pl.CostEstimate(flops=2 * rows * k * n, bytes_accessed=2 * (k * n + rows * k), transcendentals=0),
        compiler_params=pltpu.CompilerParams(vmem_limit_bytes=VMEM),
    )(*blocks, weight, cos_t, sin_t)


def first_norm_kernel(a_ref, b_ref, g_ref, h_ref, n_ref):
    part = a_ref.shape[0]
    for i, r in enumerate((a_ref, b_ref)):
        rows = slice(i * part, (i + 1) * part)
        h_ref[rows] = r[...]
        wide = r[...].astype(jnp.float32)
        inv_rms = lax.rsqrt(jnp.mean(wide * wide, axis=-1, keepdims=True) + EPS)
        n_ref[rows] = (wide * inv_rms * g_ref[...]).astype(jnp.bfloat16)


def first_norm(a, b, gain):
    part, n = a.shape
    return pl.pallas_call(
        first_norm_kernel,
        out_shape=[jax.ShapeDtypeStruct((2 * part, n), jnp.bfloat16)] * 2,
        cost_estimate=pl.CostEstimate(flops=10 ** 8, bytes_accessed=12 * part * n, transcendentals=0),
        compiler_params=pltpu.CompilerParams(vmem_limit_bytes=30 << 20),
        name="first_norm",
    )(a, b, gain.astype(jnp.float32)[None])


def flash_kernel(chunk, windowed, n_rel, part, group, nh, scale, *refs):
    sc_ref, q_ref = refs[:2]
    count = CHUNKS * n_rel
    kv_in = refs[2:2 + nh * count]
    o_ref, kv_ref, m_ref, l_ref, acc_ref, sem = refs[2 + nh * count:]
    keys = 512 if windowed else 1024
    tile = pl.program_id(0)
    here, mine, cut1, cut2 = sc_ref[0], sc_ref[1], sc_ref[2], sc_ref[3]
    rows = part * CHUNKS

    @pl.when(tile == 0)
    def _():
        copies = []
        for g in range(nh):
            for c in range(CHUNKS):
                for rel in range(n_rel):
                    i = (g * CHUNKS + c) * n_rel + rel
                    for slot, flip in enumerate((0, 2, 1, 3)):
                        dst = pl.multiple_of(rel * 4 * rows + (mine ^ flip) * rows + c * part, part)
                        copies.append(pltpu.make_async_copy(kv_in[i].at[pl.ds(slot * part, part)], kv_ref.at[g, pl.ds(dst, part)], sem.at[4 * i + slot]))
        for c in copies:
            c.start()
        for c in copies:
            c.wait()

    m_ref[...] = jnp.full(m_ref.shape, NEG, jnp.float32)
    l_ref[...] = jnp.zeros(l_ref.shape, jnp.float32)
    acc_ref[...] = jnp.zeros(acc_ref.shape, jnp.float32)
    flip = 2 * (tile % 2) + tile // 2
    tok0 = here * 4 * rows + (mine ^ flip) * rows + chunk * part

    def lowest(tok):
        low = jnp.where(tok >= cut2, cut2, jnp.where(tok >= cut1, cut1, 0))
        return jnp.maximum(low, tok - (WINDOW - 1)) if windowed else low

    first, last = lowest(tok0) // keys, tok0 // keys
    tok = tok0 + lax.broadcasted_iota(jnp.int32, (part, HEAD), 0)
    lane = lax.broadcasted_iota(jnp.int32, (part, HEAD), 1)
    lower, upper = lowest(tok) - lane, tok - lane
    chains = m_ref.shape[0]
    heads = nh * group // chains

    def body(blk, carry):
        per = 4 * rows // keys
        start = pl.multiple_of((here - blk // per) * 4 * rows + (blk % per) * keys, keys)
        bias = []
        for i in range(keys // HEAD):
            base = blk * keys + i * HEAD
            bias.append(jnp.where((lower <= base) & (upper >= base), 0.0, NEG))
        bias = jnp.concatenate(bias, axis=1)
        scores, weights = [], []
        for j in range(chains):
            kb = kv_ref[j * nh // chains, pl.ds(start, keys), :HEAD]
            qs = jnp.concatenate([q_ref[:, h * HEAD:(h + 1) * HEAD] for h in range(j * heads, (j + 1) * heads)], axis=0)
            s = lax.dot_general(qs, kb, (((1,), (1,)), ((), ())), preferred_element_type=jnp.float32)
            scores.append((s.reshape(heads, part, keys) + bias[None]).reshape(heads * part, keys))
        for j in range(chains):
            m_old = m_ref[j]
            m_new = jnp.maximum(m_old, jnp.max(scores[j], axis=1, keepdims=True))
            alpha = jnp.exp2((m_old - m_new) * scale)
            p = jnp.exp2((scores[j] - jnp.concatenate([m_new] * (keys // HEAD), axis=1)) * scale)
            total = p[:, :HEAD]
            for i in range(1, keys // HEAD):
                total = total + p[:, i * HEAD:(i + 1) * HEAD]
            l_ref[j] = alpha * l_ref[j] + total
            m_ref[j] = m_new
            weights.append((alpha, p.astype(jnp.bfloat16)))
        for j in range(chains):
            alpha, p = weights[j]
            vb = kv_ref[j * nh // chains, pl.ds(start, keys), HEAD:]
            acc_ref[j] = alpha * acc_ref[j] + jnp.dot(p, vb, preferred_element_type=jnp.float32)
        return carry

    lax.fori_loop(first, last + 1, body, 0)
    for j in range(chains):
        out = (acc_ref[j] / jnp.sum(l_ref[j], axis=1, keepdims=True)).astype(jnp.bfloat16)
        for h in range(heads):
            o_ref[:, (j * heads + h) * HEAD:(j * heads + h + 1) * HEAD] = out[h * part:(h + 1) * part]


def flash(q, kv_pieces, scalars, chunk, windowed, head, kv_heads):
    rows = q.shape[0]
    nh = len(kv_pieces)
    width = q.shape[1] * nh // kv_heads
    flat = [p for pieces in kv_pieces for p in pieces]
    n_rel = len(kv_pieces[0]) // CHUNKS
    group = width // HEAD // nh
    part = rows // 4
    state = pltpu.VMEM((2, nh * group * part // 2, HEAD), jnp.float32)
    return pl.pallas_call(
        functools.partial(flash_kernel, chunk, windowed, n_rel, part, group, nh, HEAD ** -0.5 * LOG2E),
        grid_spec=pltpu.PrefetchScalarGridSpec(
            num_scalar_prefetch=1,
            grid=(4,),
            in_specs=[pl.BlockSpec((part, width), lambda i, s: (i, head))] + [pl.BlockSpec(memory_space=pl.ANY)] * len(flat),
            out_specs=pl.BlockSpec((part, width), lambda i, s: (i, 0)),
            scratch_shapes=[
                pltpu.VMEM((nh, CHUNKS * n_rel * rows, 2 * HEAD), jnp.bfloat16),
                state, state, state,
                pltpu.SemaphoreType.DMA((4 * len(flat),)),
            ],
        ),
        out_shape=jax.ShapeDtypeStruct((rows, width), jnp.bfloat16),
        cost_estimate=pl.CostEstimate(flops=10 ** 10, bytes_accessed=4 * rows * width, transcendentals=0),
        compiler_params=pltpu.CompilerParams(vmem_limit_bytes=VMEM),
        name="flash",
    )(scalars, q, *flat)


def out_kernel(n_in, *refs):
    w_ref, o_refs = refs[n_in], refs[n_in + 1:]
    x = jnp.concatenate([r[...] for r in refs[:n_in]], axis=1)
    t = jnp.dot(x, w_ref[0], preferred_element_type=jnp.float32).astype(jnp.bfloat16)
    rows = t.shape[0] // len(o_refs)
    for i, o in enumerate(o_refs):
        o[...] = t[i * rows:(i + 1) * rows]


def project_out(mixed, weight, layer):
    rows = mixed[0].shape[0]
    k, n = weight.shape[1:]
    bn = 1024
    part = rows // 2
    return pl.pallas_call(
        functools.partial(out_kernel, len(mixed)),
        grid=(n // bn,),
        in_specs=[pl.BlockSpec(m.shape, lambda j: (0, 0)) for m in mixed] + [pl.BlockSpec((1, k, bn), lambda j: (layer, 0, j))],
        out_specs=[pl.BlockSpec((part, bn), lambda j: (0, j))] * 2,
        out_shape=[jax.ShapeDtypeStruct((part, n), jnp.bfloat16)] * 2,
        cost_estimate=pl.CostEstimate(flops=2 * rows * k * n, bytes_accessed=2 * (k * n + rows * k), transcendentals=0),
        compiler_params=pltpu.CompilerParams(vmem_limit_bytes=VMEM),
        name="out_proj",
    )(*mixed, weight)


def mlp_kernel(*refs):
    xs, (wg_ref, wu_ref, wd_ref), os, acc_ref = refs[:2], refs[2:5], refs[5:7], refs[7]
    step = pl.program_id(0)
    x = jnp.concatenate([r[...] for r in xs], axis=0)
    gate = jnp.dot(x, wg_ref[0], preferred_element_type=jnp.float32)
    up = jnp.dot(x, wu_ref[0], preferred_element_type=jnp.float32)
    act = (jax.nn.silu(gate) * up).astype(jnp.bfloat16)
    n = wd_ref.shape[2]
    bn = 1024
    part = x.shape[0] // 2
    last = pl.num_programs(0) - 1

    def each(fn):
        for c in range(0, n, bn):
            fn(slice(c, c + bn), jnp.dot(act, wd_ref[0, :, c:c + bn], preferred_element_type=jnp.float32))

    @pl.when(step == 0)
    def _():
        def put(cols, t):
            acc_ref[:, cols] = t

        each(put)

    @pl.when((step > 0) & (step < last))
    def _():
        def put(cols, t):
            acc_ref[:, cols] += t

        each(put)

    @pl.when(step == last)
    def _():
        def put(cols, t):
            t = (acc_ref[:, cols] + t).astype(jnp.bfloat16)
            for i, o in enumerate(os):
                o[:, cols] = t[i * part:(i + 1) * part]

        each(put)


def mlp(blocks, wg, wu, wd, layer):
    part, k = blocks[0].shape
    rows = 2 * part
    ff = wg.shape[2]
    n = wd.shape[2]
    bf = 256
    return pl.pallas_call(
        mlp_kernel,
        grid=(ff // bf,),
        in_specs=[pl.BlockSpec((part, k), lambda j: (0, 0))] * 2
        + [pl.BlockSpec((1, k, bf), lambda j: (layer, 0, j))] * 2
        + [pl.BlockSpec((1, bf, n), lambda j: (layer, j, 0))],
        out_specs=[pl.BlockSpec((part, n), lambda j: (0, 0))] * 2,
        out_shape=[jax.ShapeDtypeStruct((part, n), jnp.bfloat16)] * 2,
        scratch_shapes=[pltpu.VMEM((rows, n), jnp.float32)],
        cost_estimate=pl.CostEstimate(flops=6 * rows * k * ff, bytes_accessed=6 * k * ff, transcendentals=rows * ff),
        compiler_params=pltpu.CompilerParams(vmem_limit_bytes=58 << 20),
        name="mlp",
    )(*blocks, wg, wu, wd)


def solution(mesh):
    tp_size, sp_size = mesh.shape["tp"], mesh.shape["sp"]
    row_spec = P(("dp", "sp", "tp"), None)
    id_spec = P(("dp", "sp", "tp"))
    whole = P()
    in_specs = (row_spec, id_spec, id_spec, whole, P(None, None, "tp", None), whole, whole, P(None, "tp", None, None), whole, P(None, None, "tp"), P(None, None, "tp"), P(None, "tp", None))
    near = [(i, i ^ 1) for i in range(tp_size)]
    across = [(i, i ^ 2) for i in range(tp_size)]

    def local_fn(x, segment_ids, positions, g_attn, w_q, w_k, w_v, w_o, g_mlp, w_gate, w_up, w_down):
        sp_idx = lax.axis_index("sp")
        tp_idx = lax.axis_index("tp")
        layers, model, heads_loc, _ = w_q.shape
        kv_heads = w_k.shape[2] // tp_size
        rows = x.shape[0]
        part = rows // CHUNKS
        group_rows = rows * tp_size
        order = [tp_idx, tp_idx ^ 2, tp_idx ^ 1, tp_idx ^ 3]
        which = tp_idx.astype(jnp.int32)[None]

        ids = lax.all_gather(jnp.stack([segment_ids, positions]), ("sp", "tp"))
        x, ids = lax.optimization_barrier((x, ids))
        own = [x[c * part:(c + 1) * part] for c in range(CHUNKS)]
        resid, normed = [], []
        for c in range(CHUNKS):
            other = lax.ppermute(own[c], "tp", across)
            pair = first_norm(own[c], other, g_attn[0])
            resid.append(pair[0])
            normed.append(pair[1])

        seg_all = ids[:, 0].reshape(-1)
        starts = [jnp.sum((seg_all < s).astype(jnp.int32)) for s in (1, 2)]
        pos_here = lax.dynamic_slice_in_dim(ids[:, 1], sp_idx * tp_size, tp_size, 0)
        half = HEAD // 2
        inv_freq = ROPE_BASE ** (-jnp.arange(half, dtype=jnp.float32) / half)
        inv_freq = jnp.concatenate([inv_freq, inv_freq])
        sign = jnp.where(jnp.arange(HEAD) < half, -1.0, 1.0)
        cos_t, sin_t = [], []
        pos_rel = jnp.concatenate([lax.dynamic_slice_in_dim(pos_here, o, 1, 0) for o in order])
        for c in range(CHUNKS):
            pos = pos_rel[:, c * part:(c + 1) * part].reshape(-1)
            angles = pos.astype(jnp.float32)[:, None] * inv_freq[None, :]
            cos_t.append(jnp.cos(angles))
            sin_t.append(jnp.sin(angles) * sign[None, :])
        scalars = jnp.stack([sp_idx.astype(jnp.int32), tp_idx.astype(jnp.int32)] + starts)

        wo_flat = w_o.reshape(layers, heads_loc * HEAD, model)
        wq_l, wkv_l = [], []
        for layer in range(layers):
            a, b = relayout(w_q, w_k, w_v, which, layer, kv_heads)
            wq_l.append(a)
            wkv_l.append(b)

        def share(n):
            return [n, lax.ppermute(n, "tp", near)]

        def exchange(parts):
            theirs = lax.ppermute(parts[1], "tp", near)
            s = add_round(parts[0], theirs)
            return s, lax.ppermute(s, "tp", across)

        def exchange_last(parts, x_blk):
            theirs = lax.ppermute(parts[1], "tp", near)
            s = add_round(parts[0], theirs)
            r = lax.ppermute(s[part:], "tp", across)
            return add_round(x_blk[:part], add_round(s[:part], r))

        out = []
        for layer in range(layers):
            windowed = layer % 2 == 0
            shifts = min(WINDOW // group_rows, sp_size - 1) if windowed else sp_size - 1
            q, kv = [], [[] for _ in range(kv_heads)]
            for c in range(CHUNKS):
                full = share(normed[c])
                mine = project(kv_kernel, full, wkv_l[layer], cos_t[c], sin_t[c], kv_heads)
                for h in range(kv_heads):
                    kv[h].append(mine[h])
                    for s in range(1, shifts + 1):
                        kv[h].append(lax.ppermute(mine[h], "sp", [(z, z + s) for z in range(sp_size - s)]))
                q.append(project(q_kernel, full, wq_l[layer], cos_t[c], sin_t[c], 1))
            for c in range(CHUNKS):
                mixed = []
                for h in range(1 if windowed else kv_heads):
                    mixed.append(flash(q[c], kv if windowed else [kv[h]], scalars, c, windowed, h, kv_heads))
                parts = project_out(mixed, wo_flat, layer)
                s, r = exchange(parts)
                resid[c], normed[c] = residual_norm(resid[c], s, r, g_mlp[layer])
            for c in range(CHUNKS):
                full = share(normed[c])
                parts = mlp(full, w_gate, w_up, w_down, layer)
                if layer == layers - 1:
                    out.append(exchange_last(parts, resid[c]))
                else:
                    s, r = exchange(parts)
                    resid[c], normed[c] = residual_norm(resid[c], s, r, g_attn[layer + 1])
        return jnp.concatenate(out, axis=0)

    return jax.shard_map(local_fn, mesh=mesh, in_specs=in_specs, out_specs=row_spec, check_vma=False)
```

```python
import functools

import jax
import jax.numpy as jnp
from jax import lax
from jax.experimental import pallas as pl
from jax.experimental.pallas import tpu as pltpu
from jax.sharding import PartitionSpec as P


EPS = 1e-6
ROPE_BASE = 10000.0
WINDOW = 1024
HEAD = 128
CHUNKS = 2
VMEM = 40 << 20
NEG = -1e30
LOG2E = 1.4426950408889634


def add_round(a, b):
    return (a.astype(jnp.float32) + b.astype(jnp.float32)).astype(jnp.bfloat16)


def relayout_kernel(sc_ref, wq_ref, wk_ref, wv_ref, q_ref, kv_ref, tmp_ref):
    q_ref[...] = pltpu.einshape("khd->k(hd)", wq_ref[0])
    width = kv_ref.shape[1] // 2
    start = pl.multiple_of(sc_ref[0] * width, width)
    for i, w in enumerate((wk_ref, wv_ref)):
        tmp_ref[i] = pltpu.einshape("khd->k(hd)", w[0])
        part = tmp_ref[i, :, pl.ds(start, width)]
        for h in range(width // HEAD):
            at = (2 * h + i) * HEAD
            kv_ref[:, at:at + HEAD] = part[:, h * HEAD:(h + 1) * HEAD]


def relayout(w_q, w_k, w_v, which, layer, kv_loc):
    _, k, heads, _ = w_q.shape
    kv_heads = w_k.shape[2]
    bk = 256
    return pl.pallas_call(
        relayout_kernel,
        grid_spec=pltpu.PrefetchScalarGridSpec(
            num_scalar_prefetch=1,
            grid=(k // bk,),
            in_specs=[pl.BlockSpec((1, bk, heads, HEAD), lambda i, s: (layer, i, 0, 0))]
            + [pl.BlockSpec((1, bk, kv_heads, HEAD), lambda i, s: (layer, i, 0, 0))] * 2,
            out_specs=[pl.BlockSpec((bk, heads * HEAD), lambda i, s: (i, 0)), pl.BlockSpec((bk, 2 * kv_loc * HEAD), lambda i, s: (i, 0))],
            scratch_shapes=[pltpu.VMEM((2, bk, kv_heads * HEAD), jnp.bfloat16)],
        ),
        out_shape=[jax.ShapeDtypeStruct((k, heads * HEAD), jnp.bfloat16), jax.ShapeDtypeStruct((k, 2 * kv_loc * HEAD), jnp.bfloat16)],
        cost_estimate=pl.CostEstimate(flops=10 ** 10, bytes_accessed=8 * k * heads * HEAD, transcendentals=0),
        compiler_params=pltpu.CompilerParams(vmem_limit_bytes=VMEM),
        name="relayout",
    )(which, w_q, w_k, w_v)


def norm_kernel(x_ref, s_ref, r_ref, g_ref, h_ref, n_ref):
    total = (s_ref[...].astype(jnp.float32) + r_ref[...].astype(jnp.float32)).astype(jnp.bfloat16)
    h = (x_ref[...].astype(jnp.float32) + total.astype(jnp.float32)).astype(jnp.bfloat16)
    h_ref[...] = h
    wide = h.astype(jnp.float32)
    inv_rms = lax.rsqrt(jnp.mean(wide * wide, axis=-1, keepdims=True) + EPS)
    n_ref[...] = (wide * inv_rms * g_ref[...]).astype(jnp.bfloat16)


def residual_norm(x, s, r, gain):
    rows, n = x.shape
    part = rows // 2
    here = pl.BlockSpec((part, n), lambda i: (i, 0))
    return pl.pallas_call(
        norm_kernel,
        grid=(2,),
        in_specs=[here, here, pl.BlockSpec((part, n), lambda i: (1 - i, 0)), pl.BlockSpec((1, n), lambda i: (0, 0))],
        out_specs=[here, here],
        out_shape=[jax.ShapeDtypeStruct((rows, n), jnp.bfloat16)] * 2,
        cost_estimate=pl.CostEstimate(flops=10 ** 8, bytes_accessed=10 * rows * n, transcendentals=0),
        compiler_params=pltpu.CompilerParams(vmem_limit_bytes=30 << 20),
        name="residual_norm",
    )(x, s, r, gain.astype(jnp.float32)[None])


def rotate(t, cos, sin):
    wide = t.astype(jnp.float32)
    return (wide * cos + pltpu.roll(wide, HEAD // 2, 1) * sin).astype(jnp.bfloat16)


def q_kernel(*refs):
    xs, (w_ref, cos_ref, sin_ref, o_ref) = refs[:2], refs[2:]
    x = jnp.concatenate([r[...] for r in xs], axis=0)
    t = jnp.dot(x, w_ref[...], preferred_element_type=jnp.float32).astype(jnp.bfloat16)
    for h in range(t.shape[1] // HEAD):
        cols = slice(h * HEAD, (h + 1) * HEAD)
        o_ref[:, cols] = rotate(t[:, cols], cos_ref[...], sin_ref[...])


def kv_kernel(split, *refs):
    xs, (w_ref, cos_ref, sin_ref), os = refs[:2], refs[2:5], refs[5:]
    step = pl.program_id(0)
    x = jnp.concatenate([r[...] for r in xs], axis=0)
    t = jnp.dot(x, w_ref[...], preferred_element_type=jnp.float32).astype(jnp.bfloat16)
    k = rotate(t[:, :HEAD], cos_ref[...], sin_ref[...])
    if not split:
        os[0][:, :HEAD] = k
        os[0][:, HEAD:] = t[:, HEAD:]
        return
    for h, o in enumerate(os):
        @pl.when(step == h)
        def _():
            o[:, :HEAD] = k
            o[:, HEAD:] = t[:, HEAD:]


def project(kernel, blocks, weight, cos_t, sin_t, outs):
    rows = sum(b.shape[0] for b in blocks)
    k, n = weight.shape
    bn = 2 * HEAD
    if outs == 1:
        out_specs = pl.BlockSpec((rows, bn), lambda j: (0, j))
        out_shape = jax.ShapeDtypeStruct((rows, n), jnp.bfloat16)
    else:
        out_specs = [pl.BlockSpec((rows, bn), lambda j: (0, 0))] * outs
        out_shape = [jax.ShapeDtypeStruct((rows, bn), jnp.bfloat16)] * outs
    return pl.pallas_call(
        kernel,
        grid=(n // bn,),
        in_specs=[pl.BlockSpec(b.shape, lambda j: (0, 0)) for b in blocks]
        + [pl.BlockSpec((k, bn), lambda j: (0, j))]
        + [pl.BlockSpec(cos_t.shape, lambda j: (0, 0))] * 2,
        out_specs=out_specs,
        out_shape=out_shape,
        cost_estimate=pl.CostEstimate(flops=2 * rows * k * n, bytes_accessed=2 * (k * n + rows * k), transcendentals=0),
        compiler_params=pltpu.CompilerParams(vmem_limit_bytes=VMEM),
    )(*blocks, weight, cos_t, sin_t)


def first_norm_kernel(a_ref, b_ref, g_ref, h_ref, n_ref):
    part = a_ref.shape[0]
    for i, r in enumerate((a_ref, b_ref)):
        rows = slice(i * part, (i + 1) * part)
        h_ref[rows] = r[...]
        wide = r[...].astype(jnp.float32)
        inv_rms = lax.rsqrt(jnp.mean(wide * wide, axis=-1, keepdims=True) + EPS)
        n_ref[rows] = (wide * inv_rms * g_ref[...]).astype(jnp.bfloat16)


def first_norm(a, b, gain):
    part, n = a.shape
    return pl.pallas_call(
        first_norm_kernel,
        out_shape=[jax.ShapeDtypeStruct((2 * part, n), jnp.bfloat16)] * 2,
        cost_estimate=pl.CostEstimate(flops=10 ** 8, bytes_accessed=12 * part * n, transcendentals=0),
        compiler_params=pltpu.CompilerParams(vmem_limit_bytes=30 << 20),
        name="first_norm",
    )(a, b, gain.astype(jnp.float32)[None])


def flash_kernel(cols, chunk, windowed, n_rel, part, group, nh, scale, *refs):
    sc_ref, q_ref = refs[:2]
    kv_in = refs[2:2 + len(cols)]
    o_ref, kv_ref, m_ref, l_ref, acc_ref, sem = refs[2 + len(cols):]
    keys = 512 if windowed else 1024
    tile = pl.program_id(0)
    here, mine, cut1, cut2 = sc_ref[0], sc_ref[1], sc_ref[2], sc_ref[3]
    rows = part * CHUNKS

    @pl.when(tile == 0)
    def _():
        copies = []
        for g in range(nh):
            for c in range(CHUNKS):
                for rel in range(n_rel):
                    i = (g * CHUNKS + c) * n_rel + rel
                    for slot, flip in enumerate((0, 2, 1, 3)):
                        dst = pl.multiple_of(rel * 4 * rows + (mine ^ flip) * rows + c * part, part)
                        copies.append(pltpu.make_async_copy(kv_in[i].at[pl.ds(slot * part, part), pl.ds(cols[i] * 2 * HEAD, 2 * HEAD)], kv_ref.at[g, pl.ds(dst, part)], sem.at[4 * i + slot]))
        for c in copies:
            c.start()
        for c in copies:
            c.wait()

    m_ref[...] = jnp.full(m_ref.shape, NEG, jnp.float32)
    l_ref[...] = jnp.zeros(l_ref.shape, jnp.float32)
    acc_ref[...] = jnp.zeros(acc_ref.shape, jnp.float32)
    flip = 2 * (tile % 2) + tile // 2
    tok0 = here * 4 * rows + (mine ^ flip) * rows + chunk * part

    def lowest(tok):
        low = jnp.where(tok >= cut2, cut2, jnp.where(tok >= cut1, cut1, 0))
        return jnp.maximum(low, tok - (WINDOW - 1)) if windowed else low

    first, last = lowest(tok0) // keys, tok0 // keys
    tok = tok0 + lax.broadcasted_iota(jnp.int32, (part, HEAD), 0)
    lane = lax.broadcasted_iota(jnp.int32, (part, HEAD), 1)
    lower, upper = lowest(tok) - lane, tok - lane
    chains = m_ref.shape[0]
    heads = nh * group // chains

    def body(blk, carry):
        per = 4 * rows // keys
        start = pl.multiple_of((here - blk // per) * 4 * rows + (blk % per) * keys, keys)
        bias = []
        for i in range(keys // HEAD):
            base = blk * keys + i * HEAD
            bias.append(jnp.where((lower <= base) & (upper >= base), 0.0, NEG))
        bias = jnp.concatenate(bias, axis=1)
        scores, weights = [], []
        for j in range(chains):
            kb = kv_ref[j * nh // chains, pl.ds(start, keys), :HEAD]
            qs = jnp.concatenate([q_ref[:, h * HEAD:(h + 1) * HEAD] for h in range(j * heads, (j + 1) * heads)], axis=0)
            s = lax.dot_general(qs, kb, (((1,), (1,)), ((), ())), preferred_element_type=jnp.float32)
            scores.append((s.reshape(heads, part, keys) + bias[None]).reshape(heads * part, keys))
        for j in range(chains):
            m_old = m_ref[j]
            m_new = jnp.maximum(m_old, jnp.max(scores[j], axis=1, keepdims=True))
            alpha = jnp.exp2((m_old - m_new) * scale)
            p = jnp.exp2((scores[j] - jnp.concatenate([m_new] * (keys // HEAD), axis=1)) * scale)
            total = p[:, :HEAD]
            for i in range(1, keys // HEAD):
                total = total + p[:, i * HEAD:(i + 1) * HEAD]
            l_ref[j] = alpha * l_ref[j] + total
            m_ref[j] = m_new
            weights.append((alpha, p.astype(jnp.bfloat16)))
        for j in range(chains):
            alpha, p = weights[j]
            vb = kv_ref[j * nh // chains, pl.ds(start, keys), HEAD:]
            acc_ref[j] = alpha * acc_ref[j] + jnp.dot(p, vb, preferred_element_type=jnp.float32)
        return carry

    lax.fori_loop(first, last + 1, body, 0)
    for j in range(chains):
        out = (acc_ref[j] / jnp.sum(l_ref[j], axis=1, keepdims=True)).astype(jnp.bfloat16)
        for h in range(heads):
            o_ref[:, (j * heads + h) * HEAD:(j * heads + h + 1) * HEAD] = out[h * part:(h + 1) * part]


def flash(q, kv_pieces, scalars, chunk, windowed, head, kv_heads):
    rows = q.shape[0]
    nh = len(kv_pieces)
    width = q.shape[1] * nh // kv_heads
    flat = [p[0] for pieces in kv_pieces for p in pieces]
    cols = tuple(p[1] for pieces in kv_pieces for p in pieces)
    n_rel = len(kv_pieces[0]) // CHUNKS
    group = width // HEAD // nh
    part = rows // 4
    state = pltpu.VMEM((2, nh * group * part // 2, HEAD), jnp.float32)
    return pl.pallas_call(
        functools.partial(flash_kernel, cols, chunk, windowed, n_rel, part, group, nh, HEAD ** -0.5 * LOG2E),
        grid_spec=pltpu.PrefetchScalarGridSpec(
            num_scalar_prefetch=1,
            grid=(4,),
            in_specs=[pl.BlockSpec((part, width), lambda i, s: (i, head))] + [pl.BlockSpec(memory_space=pl.ANY)] * len(flat),
            out_specs=pl.BlockSpec((part, width), lambda i, s: (i, 0)),
            scratch_shapes=[
                pltpu.VMEM((nh, CHUNKS * n_rel * rows, 2 * HEAD), jnp.bfloat16),
                state, state, state,
                pltpu.SemaphoreType.DMA((4 * len(flat),)),
            ],
        ),
        out_shape=jax.ShapeDtypeStruct((rows, width), jnp.bfloat16),
        cost_estimate=pl.CostEstimate(flops=10 ** 10, bytes_accessed=4 * rows * width, transcendentals=0),
        compiler_params=pltpu.CompilerParams(vmem_limit_bytes=VMEM),
        name="flash",
    )(scalars, q, *flat)


def out_kernel(n_in, *refs):
    w_ref, o_refs = refs[n_in], refs[n_in + 1:]
    x = jnp.concatenate([r[...] for r in refs[:n_in]], axis=1)
    t = jnp.dot(x, w_ref[0], preferred_element_type=jnp.float32).astype(jnp.bfloat16)
    rows = t.shape[0] // len(o_refs)
    for i, o in enumerate(o_refs):
        o[...] = t[i * rows:(i + 1) * rows]


def project_out(mixed, weight, layer):
    rows = mixed[0].shape[0]
    k, n = weight.shape[1:]
    bn = 1024
    part = rows // 2
    return pl.pallas_call(
        functools.partial(out_kernel, len(mixed)),
        grid=(n // bn,),
        in_specs=[pl.BlockSpec(m.shape, lambda j: (0, 0)) for m in mixed] + [pl.BlockSpec((1, k, bn), lambda j: (layer, 0, j))],
        out_specs=[pl.BlockSpec((part, bn), lambda j: (0, j))] * 2,
        out_shape=[jax.ShapeDtypeStruct((part, n), jnp.bfloat16)] * 2,
        cost_estimate=pl.CostEstimate(flops=2 * rows * k * n, bytes_accessed=2 * (k * n + rows * k), transcendentals=0),
        compiler_params=pltpu.CompilerParams(vmem_limit_bytes=VMEM),
        name="out_proj",
    )(*mixed, weight)


def mlp_kernel(*refs):
    xs, (wg_ref, wu_ref, wd_ref), os, acc_ref = refs[:2], refs[2:5], refs[5:7], refs[7]
    step = pl.program_id(0)
    x = jnp.concatenate([r[...] for r in xs], axis=0)
    gate = jnp.dot(x, wg_ref[0], preferred_element_type=jnp.float32)
    up = jnp.dot(x, wu_ref[0], preferred_element_type=jnp.float32)
    act = (jax.nn.silu(gate) * up).astype(jnp.bfloat16)
    n = wd_ref.shape[2]
    bn = 1024
    part = x.shape[0] // 2
    last = pl.num_programs(0) - 1

    def each(fn):
        for c in range(0, n, bn):
            fn(slice(c, c + bn), jnp.dot(act, wd_ref[0, :, c:c + bn], preferred_element_type=jnp.float32))

    @pl.when(step == 0)
    def _():
        def put(cols, t):
            acc_ref[:, cols] = t

        each(put)

    @pl.when((step > 0) & (step < last))
    def _():
        def put(cols, t):
            acc_ref[:, cols] += t

        each(put)

    @pl.when(step == last)
    def _():
        def put(cols, t):
            t = (acc_ref[:, cols] + t).astype(jnp.bfloat16)
            for i, o in enumerate(os):
                o[:, cols] = t[i * part:(i + 1) * part]

        each(put)


def mlp(blocks, wg, wu, wd, layer):
    part, k = blocks[0].shape
    rows = 2 * part
    ff = wg.shape[2]
    n = wd.shape[2]
    bf = 256
    return pl.pallas_call(
        mlp_kernel,
        grid=(ff // bf,),
        in_specs=[pl.BlockSpec((part, k), lambda j: (0, 0))] * 2
        + [pl.BlockSpec((1, k, bf), lambda j: (layer, 0, j))] * 2
        + [pl.BlockSpec((1, bf, n), lambda j: (layer, j, 0))],
        out_specs=[pl.BlockSpec((part, n), lambda j: (0, 0))] * 2,
        out_shape=[jax.ShapeDtypeStruct((part, n), jnp.bfloat16)] * 2,
        scratch_shapes=[pltpu.VMEM((rows, n), jnp.float32)],
        cost_estimate=pl.CostEstimate(flops=6 * rows * k * ff, bytes_accessed=6 * k * ff, transcendentals=rows * ff),
        compiler_params=pltpu.CompilerParams(vmem_limit_bytes=58 << 20),
        name="mlp",
    )(*blocks, wg, wu, wd)


def solution(mesh):
    tp_size, sp_size = mesh.shape["tp"], mesh.shape["sp"]
    row_spec = P(("dp", "sp", "tp"), None)
    id_spec = P(("dp", "sp", "tp"))
    whole = P()
    in_specs = (row_spec, id_spec, id_spec, whole, P(None, None, "tp", None), whole, whole, P(None, "tp", None, None), whole, P(None, None, "tp"), P(None, None, "tp"), P(None, "tp", None))
    near = [(i, i ^ 1) for i in range(tp_size)]
    across = [(i, i ^ 2) for i in range(tp_size)]

    def local_fn(x, segment_ids, positions, g_attn, w_q, w_k, w_v, w_o, g_mlp, w_gate, w_up, w_down):
        sp_idx = lax.axis_index("sp")
        tp_idx = lax.axis_index("tp")
        layers, model, heads_loc, _ = w_q.shape
        kv_heads = w_k.shape[2] // tp_size
        rows = x.shape[0]
        part = rows // CHUNKS
        group_rows = rows * tp_size
        which = tp_idx.astype(jnp.int32)[None]

        ids = jnp.stack([segment_ids, positions])
        far = lax.ppermute(ids, "tp", across)
        both = jnp.stack([ids, far])
        beside = lax.ppermute(both, "tp", near)
        ids = jnp.concatenate([both, beside])
        own, others = [x[c * part:(c + 1) * part] for c in range(CHUNKS)], []
        for c in range(CHUNKS):
            others.append(lax.ppermute(own[c], "tp", across))
        resid, normed = [], []
        for c in range(CHUNKS):
            pair = first_norm(own[c], others[c], g_attn[0])
            resid.append(pair[0])
            normed.append(pair[1])

        before = jnp.stack([jnp.sum((ids[:, 0] < s).astype(jnp.int32)) for s in (1, 2)])
        before = jnp.broadcast_to(before[:, None], (2, HEAD))
        for hop in (1, 2):
            far = lax.ppermute(before, "sp", [(z, z ^ hop) for z in range(sp_size)])
            before = before + far
        starts = [before[0, 0], before[1, 0]]
        half = HEAD // 2
        inv_freq = ROPE_BASE ** (-jnp.arange(half, dtype=jnp.float32) / half)
        inv_freq = jnp.concatenate([inv_freq, inv_freq])
        sign = jnp.where(jnp.arange(HEAD) < half, -1.0, 1.0)
        cos_t, sin_t = [], []
        pos_rel = ids[:, 1]
        for c in range(CHUNKS):
            pos = pos_rel[:, c * part:(c + 1) * part].reshape(-1)
            angles = pos.astype(jnp.float32)[:, None] * inv_freq[None, :]
            cos_t.append(jnp.cos(angles))
            sin_t.append(jnp.sin(angles) * sign[None, :])
        scalars = jnp.stack([sp_idx.astype(jnp.int32), tp_idx.astype(jnp.int32)] + starts)

        wo_flat = w_o.reshape(layers, heads_loc * HEAD, model)
        wq_l, wkv_l = [], []
        for layer in range(layers):
            a, b = relayout(w_q, w_k, w_v, which, layer, kv_heads)
            wq_l.append(a)
            wkv_l.append(b)

        def share(n):
            return [n, lax.ppermute(n, "tp", near)]

        def exchange(parts):
            theirs = lax.ppermute(parts[1], "tp", near)
            s = add_round(parts[0], theirs)
            return s, lax.ppermute(s, "tp", across)

        def exchange_last(parts, x_blk):
            theirs = lax.ppermute(parts[1], "tp", near)
            s = add_round(parts[0], theirs)
            r = lax.ppermute(s[part:], "tp", across)
            return add_round(x_blk[:part], add_round(s[:part], r))

        out = []
        for layer in range(layers):
            windowed = layer % 2 == 0
            shifts = min(WINDOW // group_rows, sp_size - 1) if windowed else sp_size - 1
            q, kv = [], [[] for _ in range(kv_heads)]
            for c in range(CHUNKS):
                full = share(normed[c])
                split = not windowed and c == CHUNKS - 1
                mine = project(functools.partial(kv_kernel, split), full, wkv_l[layer], cos_t[c], sin_t[c], kv_heads if split else 1)
                for h, piece in enumerate(mine if split else [mine]):
                    got = [piece]
                    for s in range(1, shifts + 1):
                        got.append(lax.ppermute(piece, "sp", [(z, z + s) for z in range(sp_size - s)]))
                    for g in [h] if split else range(kv_heads):
                        kv[g] += [(v, 0 if split else g) for v in got]
                q.append(project(q_kernel, full, wq_l[layer], cos_t[c], sin_t[c], 1))
            for c in range(CHUNKS):
                mixed = []
                for h in range(1 if windowed else kv_heads):
                    mixed.append(flash(q[c], kv if windowed else [kv[h]], scalars, c, windowed, h, kv_heads))
                parts = project_out(mixed, wo_flat, layer)
                s, r = exchange(parts)
                resid[c], normed[c] = residual_norm(resid[c], s, r, g_mlp[layer])
            for c in range(CHUNKS):
                full = share(normed[c])
                parts = mlp(full, w_gate, w_up, w_down, layer)
                if layer == layers - 1:
                    out.append(exchange_last(parts, resid[c]))
                else:
                    s, r = exchange(parts)
                    resid[c], normed[c] = residual_norm(resid[c], s, r, g_attn[layer + 1])
        return jnp.concatenate(out, axis=0)

    return jax.shard_map(local_fn, mesh=mesh, in_specs=in_specs, out_specs=row_spec, check_vma=False)
```
